32 devices in a mesh: tm: 4 (over y, x), space: 8 (over z, core).
Axes of the slice: x: 2, y: 2, z: 4, core: 2. Of those that a mesh axis runs over, the one named last changes fastest.
Arguments:
- queries: bfloat16 [4096, 4096], P(('tm', 'space')), may hold values from -20 to 20
- key_vectors: bfloat16 [4096, 4096], P(('tm', 'space')), may hold values from -20 to 20
- value_vectors: bfloat16 [4096, 4096], P(('tm', 'space')), may hold values from -6 to 6
- out_weight: bfloat16 [4096, 6144], P(None, 'space'), may hold values from -0.375 to 0.375
- frame_mask: int32 [4, 4], replicated, may hold values 0 or 1
Outputs:
- projected: bfloat16 [4096, 6144], P('tm', 'space')
The draws below stay inside these ranges and needn't reach their ends.
All inputs are finite; a program needn't handle non-finite values.
Results may differ from the reference program's by a relative error of at most 0.0075.
Values may be sent and summed in bfloat16 or wider, within the bound.
A program may use at most 128 MiB of HBM per device.

```python
import math
import jax
import jax.numpy as jnp
from jax import lax

D = 6144
HD = 128
HEADS = 32
TOK_DEV = 128
WIN = 1
BLOCKS = 4
TOKENS = 4096
N_TM = 4
N_SPACE = 8


def pair_draw(key):
    base = jax.random.fold_in(key, 7193)
    first_key, second_key = jax.random.split(base, 2)
    width = HEADS * HD
    query_draw = 2.0 * jax.random.truncated_normal(first_key, -4.0, 4.0, (TOKENS, width), jnp.float32)
    key_draw = jax.random.truncated_normal(second_key, -4.0, 4.0, (TOKENS, width), jnp.float32)
    return (query_draw, key_draw)


def draw_queries(key, part):
    return pair_draw(key)[0].astype(jnp.bfloat16)


def draw_key_vectors(key, part):
    return pair_draw(key)[1].astype(jnp.bfloat16)


def set_ends(drawn, own_key, least, top_value):
    extent = drawn.shape
    index_at = [jax.random.randint(jax.random.fold_in(own_key, axis), (), 0, extent[axis]) for axis in range(len(extent))]
    drawn = drawn.at[tuple(index_at)].set(least)
    longest = extent.index(max(extent))
    index_at[longest] = (index_at[longest] + 1) % extent[longest]
    return drawn.at[tuple(index_at)].set(top_value)


def block_scale(key, dims, cuts, least, largest):
    gain, own = 1.0, jax.random.fold_in(key, 6)
    for axis_at, blocks in cuts:
        draws = jnp.exp(jax.random.uniform(jax.random.fold_in(own, axis_at), (blocks,), jnp.float32, least / len(cuts), largest / len(cuts)))
        gain = gain * jnp.repeat(draws, dims[axis_at] // blocks).reshape([-1 if axis == axis_at else 1 for axis in range(len(dims))])
    return gain


def noise(key, shape, scale, limit, shards=(), kind=jnp.bfloat16):
    drawn = scale * jax.random.normal(key, shape, jnp.float32)
    if shards:
        drawn = drawn * block_scale(key, shape, shards, -0.22, 0.18)
    return jnp.clip(drawn, -limit, limit).astype(kind)


def setup_inputs(seed: int = 0) -> dict:
    keys = jax.random.split(jax.random.key(seed), 6)
    return {
        "queries": draw_queries(jax.random.fold_in(keys[5], 71), 0),
        "key_vectors": draw_key_vectors(jax.random.fold_in(keys[5], 71), 0),
        "value_vectors": noise(keys[2], (TOKENS, HEADS * HD), 1.0, 6.0, ((0, 32),)),
        "out_weight": noise(keys[3], (HEADS * HD, D), (HEADS * HD // 16) ** -0.5, 0.375, ((1, 8),)),
        "frame_mask": set_ends((jax.random.randint(keys[4], (BLOCKS, BLOCKS), 0, 5) < 4).astype(jnp.int32), jax.random.fold_in(keys[4], 1), 0, 1),
    }


def reference(queries, key_vectors, value_vectors, out_weight, frame_mask):
    block_tokens = TOK_DEV * N_SPACE
    scale_factor = 1.0 / math.sqrt(HD)
    pieces = []
    for frame_index in range(N_TM):
        block_list = [(frame_index + offset) % N_TM for offset in range(-WIN, WIN + 1)]
        query_rows = queries[frame_index * block_tokens:(frame_index + 1) * block_tokens]
        query_rows = query_rows.reshape(block_tokens, HEADS, HD).transpose(1, 0, 2)
        key_rows = jnp.concatenate([key_vectors[b * block_tokens:(b + 1) * block_tokens] for b in block_list], axis=0)
        key_rows = key_rows.reshape(-1, HEADS, HD).transpose(1, 0, 2)
        value_rows = jnp.concatenate([value_vectors[b * block_tokens:(b + 1) * block_tokens] for b in block_list], axis=0)
        value_rows = value_rows.reshape(-1, HEADS, HD).transpose(1, 0, 2)
        owners = jnp.concatenate([jnp.full((block_tokens,), b, jnp.int32) for b in block_list])
        mask_bits = frame_mask[frame_index][owners]
        allowed = (owners == frame_index) | (mask_bits == 1)

        def one_head(head_trio):
            query_head, key_head, value_head = head_trio
            scores = jnp.dot(query_head, key_head.T, preferred_element_type=jnp.float32) * scale_factor
            scores = jnp.where(allowed[None, :], scores, -jnp.inf)
            row_top = lax.optimization_barrier(jnp.max(scores, axis=1, keepdims=True))
            exp_terms = jnp.where(allowed[None, :], jnp.exp(scores - row_top), 0.0)
            totals = lax.optimization_barrier(jnp.sum(exp_terms, axis=1, keepdims=True))
            mixed = jnp.dot(exp_terms.astype(jnp.bfloat16), value_head, preferred_element_type=jnp.float32)
            return mixed / totals
        heads_out = lax.map(one_head, (query_rows, key_rows, value_rows))
        attended = heads_out.transpose(1, 0, 2).reshape(block_tokens, HEADS * HD).astype(jnp.bfloat16)
        pieces.append(jnp.dot(attended, out_weight, preferred_element_type=jnp.float32).astype(jnp.bfloat16))
    return jnp.concatenate(pieces, axis=0)
```

```python
import functools
import math

import jax
import jax.numpy as jnp
from jax import lax
from jax.experimental import pallas as pl
from jax.experimental.pallas import tpu as pltpu
from jax.sharding import PartitionSpec as P

HD = 128
MESH = pl.DeviceIdType.MESH


def kernel(
    frames, places, heads,
    q_hbm, k_hbm, v_hbm, w_hbm, mask_ref, out_ref,
    qb, kvb, kvx, kvy, gat, wv, acc,
    a_send, a_recv, x_send, x_recv, y_send, y_recv,
    g_send, g_recv, p_recv, w_sem,
):
    f = lax.axis_index("tm")
    s = lax.axis_index("space")
    tok = q_hbm.shape[0]
    rows = tok * places
    chips = places // 2
    z = lax.div(s, 2)
    core = lax.rem(s, 2)
    odd = lax.rem(f, 2)
    partner = f + 1 - 2 * odd
    onward = lax.rem(f + 2 - 4 * odd + frames, frames)
    behind = lax.rem(f - 2 + 4 * odd + frames, frames)
    far = lax.rem(f - 1 + 2 * odd + frames, frames)
    mate = 2 * z + 1 - core

    barrier = pltpu.get_barrier_semaphore()

    def greet(j, carry):
        pl.semaphore_signal(
            barrier, inc=1, device_id=(f, lax.rem(s + j, places)), device_id_type=MESH
        )
        return carry

    lax.fori_loop(1, places, greet, 0)
    for other in (partner, onward, behind):
        pl.semaphore_signal(barrier, inc=1, device_id=(other, s), device_id_type=MESH)
    pl.semaphore_wait(barrier, places - 1 + 3)

    def remote(src, dst, send, recv, tm_to, space_to):
        return pltpu.make_async_remote_copy(
            src_ref=src, dst_ref=dst, send_sem=send, recv_sem=recv,
            device_id=(tm_to, space_to), device_id_type=MESH,
        )

    def landing(t, h):
        return qb.at[h] if t == 2 else kvb.at[t, h]

    sources = (k_hbm, v_hbm, q_hbm)

    def send_head(h):
        for t in range(3):
            mine = landing(t, h).at[pl.ds(pl.multiple_of(s * tok, tok), tok), :]

            def one(j, carry):
                to = lax.rem(s + j, places)
                cols = pl.ds(pl.multiple_of((to * heads + h) * HD, HD), HD)
                remote(
                    sources[t].at[:, cols], mine, a_send.at[h, t], a_recv.at[h, t], f, to
                ).start()
                return carry

            lax.fori_loop(1, places, one, 0)
            cols = pl.ds(pl.multiple_of((s * heads + h) * HD, HD), HD)
            pltpu.make_async_copy(sources[t].at[:, cols], mine, a_recv.at[h, t]).start()

    def whole_wait(ref, sem):
        pltpu.make_async_copy(ref, ref, sem).wait()

    def x_copy(h, t):
        return remote(
            kvb.at[t, h], kvx.at[t, h], x_send.at[h, t], x_recv.at[h, t], partner, s
        )

    def y_copy(h, t):
        return remote(
            kvx.at[t, h], kvy.at[t, h], y_send.at[h, t], y_recv.at[h, t], onward, s
        )

    def columns(place):
        return pl.ds(pl.multiple_of(place * HD, HD), HD)

    def g_copy(g, place, slot, recv, to):
        part = gat.at[g, :, columns(place)]
        return remote(part, part, g_send.at[g, slot], recv, f, to)

    def own_copies(g):
        return [
            (z < chips - 1, g_copy(g, s, 0, g_recv.at[g, 0, 0], s + 2)),
            (z > 0, g_copy(g, s, 1, g_recv.at[g, 1, 0], s - 2)),
            (None, g_copy(g, s, 2, p_recv.at[g, z], mate)),
        ]

    def relay_copies(g, k):
        low, high = s - 2 * k, s + 2 * k
        base = 3 + 4 * (k - 1)
        copies = []
        if k < chips - 1:
            copies.append(((z >= k) & (z < chips - 1),
                           lambda: g_copy(g, low, base, g_recv.at[g, 0, k], s + 2)))
        copies.append((z >= k, lambda: g_copy(g, low, base + 1, p_recv.at[g, z - k], mate)))
        if k < chips - 1:
            copies.append(((z + k <= chips - 1) & (z > 0),
                           lambda: g_copy(g, high, base + 2, g_recv.at[g, 1, k], s - 2)))
        copies.append((z + k <= chips - 1,
                       lambda: g_copy(g, high, base + 3, p_recv.at[g, z + k], mate)))
        return copies

    def start_own(g):
        for cond, copy in own_copies(g):
            if cond is None:
                copy.start()
            else:
                pl.when(cond)(copy.start)

    def relay(g, k):
        @pl.when(z >= k)
        def _():
            g_copy(g, s - 2 * k, 0, g_recv.at[g, 0, k - 1], mate).wait_recv()

        @pl.when(z + k <= chips - 1)
        def _():
            g_copy(g, s + 2 * k, 0, g_recv.at[g, 1, k - 1], mate).wait_recv()

        for cond, make in relay_copies(g, k):
            @pl.when(cond)
            def _():
                make().start()

    near_pen = jnp.where(mask_ref[f, partner] == 1, 0.0, jnp.inf).astype(jnp.float32)
    far_pen = jnp.where(mask_ref[f, far] == 1, 0.0, jnp.inf).astype(jnp.float32)
    factor = math.log2(math.e) / math.sqrt(HD)
    q_tile = min(256, rows)
    tiles = rows // q_tile

    def attend(h, first, last):
        def tile(i, carry):
            at = pl.ds(pl.multiple_of(i * q_tile, q_tile), q_tile)
            q = qb[h, at, :]
            places_kv = ((kvb, None), (kvx, near_pen), (kvy, far_pen))
            scores = []
            top = None
            for ref, pen in places_kv:
                sc = lax.dot_general(
                    q, ref[0, h], (((1,), (1,)), ((), ())),
                    preferred_element_type=jnp.float32,
                )
                scores.append(sc)
                best = jnp.max(sc, axis=1, keepdims=True)
                best = best if pen is None else best - pen
                top = best if top is None else jnp.maximum(top, best)
            total = None
            mixed = None
            for sc, (ref, pen) in zip(scores, places_kv):
                level = top if pen is None else top + pen
                e = jnp.exp2((sc - level) * factor)
                part = jnp.sum(e, axis=1, keepdims=True)
                prod = jnp.dot(
                    e.astype(jnp.bfloat16), ref[1, h], preferred_element_type=jnp.float32
                )
                total = part if total is None else total + part
                mixed = prod if mixed is None else mixed + prod
            gat[h, at, columns(s)] = (mixed / total).astype(jnp.bfloat16)
            return carry

        lax.fori_loop(first, last, tile, 0)

    p_tile = min(256, rows)

    def project(g):
        for o in range(chips):
            g_copy(g, 2 * o + 1 - core, 0, p_recv.at[g, o], mate).wait_recv()
        whole_wait(wv.at[g], w_sem.at[g])

        def tile(i, carry):
            at = pl.ds(pl.multiple_of(i * p_tile, p_tile), p_tile)
            prod = jnp.dot(gat[g, at, :], wv[g], preferred_element_type=jnp.float32)
            if g > 0:
                prod = prod + acc[at, :]
            if g == heads - 1:
                out_ref[at, :] = prod.astype(out_ref.dtype)
            else:
                acc[at, :] = prod
            return carry

        lax.fori_loop(0, rows // p_tile, tile, 0)

    events = [(g, k) for g in range(heads) for k in range(1, chips)]
    done = [0]

    def relay_some(count, limit_group):
        while count > 0 and done[0] < len(events) and events[done[0]][0] <= limit_group:
            g, k = events[done[0]]
            relay(g, k)
            done[0] += 1
            count -= 1
            if k == chips - 1 and limit_group >= heads - 1:
                project(g)

    for h in range(min(2, heads)):
        send_head(h)
    for h in range(heads):
        def load(i, carry):
            pltpu.make_async_copy(
                w_hbm.at[pl.ds(pl.multiple_of((i * heads + h) * HD, HD), HD), :],
                wv.at[h, pl.ds(pl.multiple_of(i * HD, HD), HD), :],
                w_sem.at[h],
            ).start()
            return carry

        lax.fori_loop(0, places, load, 0)

    for step in range(heads + 1):
        if step < heads:
            for t in range(2):
                whole_wait(kvb.at[t, step], a_recv.at[step, t])
                x_copy(step, t).start()
            if step + 2 < heads:
                send_head(step + 2)
            for t in range(2):
                x_copy(step, t).wait_recv()
                y_copy(step, t).start()
        h = step - 1
        if h < 0:
            continue
        if h >= 2:
            relay_some(1, h - 2)
        whole_wait(qb.at[h], a_recv.at[h, 2])
        for t in range(2):
            y_copy(h, t).wait_recv()
        if h == heads - 1:
            attend(h, 0, tiles // 2)
            relay_some(2, h - 1)
            attend(h, tiles // 2, tiles)
        else:
            attend(h, 0, tiles)
        start_own(h)
    for g in range(done[0] // (chips - 1)):
        project(g)
    relay_some(len(events), heads - 1)

    for h in range(heads):
        for t in range(3):
            part = landing(t, h).at[pl.ds(0, (places - 1) * tok), :]
            whole_wait(part, a_send.at[h, t])
        for t in range(2):
            x_copy(h, t).wait_send()
            y_copy(h, t).wait_send()
        for cond, copy in own_copies(h):
            if cond is None:
                copy.wait_send()
            else:
                pl.when(cond)(copy.wait_send)
        for k in range(1, chips):
            for cond, make in relay_copies(h, k):
                @pl.when(cond)
                def _():
                    make().wait_send()


def solution(mesh):
    frames = mesh.shape["tm"]
    places = mesh.shape["space"]

    def body(queries, key_vectors, value_vectors, out_weight, frame_mask):
        tok, width = queries.shape
        heads = width // HD // places
        rows = tok * places
        chips = places // 2
        cols = out_weight.shape[1]
        bf16 = jnp.bfloat16
        anyspace = pl.BlockSpec(memory_space=pl.ANY)
        dma = pltpu.SemaphoreType.DMA
        return pl.pallas_call(
            functools.partial(kernel, frames, places, heads),
            out_shape=jax.ShapeDtypeStruct((rows, cols), bf16),
            in_specs=[anyspace] * 4 + [pl.BlockSpec(memory_space=pltpu.SMEM)],
            out_specs=pl.BlockSpec(memory_space=pltpu.VMEM),
            scratch_shapes=[
                pltpu.VMEM((heads, rows, HD), bf16),
                pltpu.VMEM((2, heads, rows, HD), bf16),
                pltpu.VMEM((2, heads, rows, HD), bf16),
                pltpu.VMEM((2, heads, rows, HD), bf16),
                pltpu.VMEM((heads, rows, places * HD), bf16),
                pltpu.VMEM((heads, places * HD, cols), bf16),
                pltpu.VMEM((rows, cols), jnp.float32),
                dma((heads, 3)), dma((heads, 3)),
                dma((heads, 2)), dma((heads, 2)),
                dma((heads, 2)), dma((heads, 2)),
                dma((heads, 3 + 4 * (chips - 1))),
                dma((heads, 2, chips - 1)),
                dma((heads, chips)),
                dma((heads,)),
            ],
            compiler_params=pltpu.CompilerParams(
                collective_id=0, has_side_effects=True,
                vmem_limit_bytes=60 * 1024 * 1024,
            ),
        )(queries, key_vectors, value_vectors, out_weight, frame_mask)

    in_specs = (
        P(("tm", "space"), None),
        P(("tm", "space"), None),
        P(("tm", "space"), None),
        P(None, "space"),
        P(),
    )
    return jax.shard_map(
        body, mesh=mesh, in_specs=in_specs, out_specs=P("tm", "space"), check_vma=False
    )
```

```python
import functools
import math

import jax
import jax.numpy as jnp
from jax import lax
from jax.experimental import pallas as pl
from jax.experimental.pallas import tpu as pltpu
from jax.sharding import PartitionSpec as P

HD = 128
MESH = pl.DeviceIdType.MESH


def kernel(
    frames, places, heads,
    q_hbm, k_hbm, v_hbm, w_hbm, mask_ref, out_ref,
    qb, kvb, kvx, kvy, gat, wv, acc,
    a_send, a_recv, x_send, x_recv, y_send, y_recv,
    g_send, g_recv, p_recv, w_sem,
):
    f = lax.axis_index("tm")
    s = lax.axis_index("space")
    tok = q_hbm.shape[0]
    rows = tok * places
    half = rows // 2
    chips = places // 2
    z = lax.div(s, 2)
    core = lax.rem(s, 2)
    odd = lax.rem(f, 2)
    partner = f + 1 - 2 * odd
    onward = lax.rem(f + 2 - 4 * odd + frames, frames)
    behind = lax.rem(f - 2 + 4 * odd + frames, frames)
    far = lax.rem(f - 1 + 2 * odd + frames, frames)
    mate = 2 * z + 1 - core

    barrier = pltpu.get_barrier_semaphore()

    def greet(j, carry):
        pl.semaphore_signal(
            barrier, inc=1, device_id=(f, lax.rem(s + j, places)), device_id_type=MESH
        )
        return carry

    lax.fori_loop(1, places, greet, 0)
    for other in (partner, onward, behind):
        pl.semaphore_signal(barrier, inc=1, device_id=(other, s), device_id_type=MESH)
    pl.semaphore_wait(barrier, places - 1 + 3)

    def remote(src, dst, send, recv, tm_to, space_to):
        return pltpu.make_async_remote_copy(
            src_ref=src, dst_ref=dst, send_sem=send, recv_sem=recv,
            device_id=(tm_to, space_to), device_id_type=MESH,
        )

    def landing(t, h):
        return qb.at[h] if t == 2 else kvb.at[t, h]

    sources = (k_hbm, v_hbm, q_hbm)

    def send_head(h):
        for t in range(3):
            mine = landing(t, h).at[pl.ds(pl.multiple_of(s * tok, tok), tok), :]

            def one(j, carry):
                to = lax.rem(s + j, places)
                cols = pl.ds(pl.multiple_of((to * heads + h) * HD, HD), HD)
                remote(
                    sources[t].at[:, cols], mine, a_send.at[h, t], a_recv.at[h, t], f, to
                ).start()
                return carry

            lax.fori_loop(1, places, one, 0)
            cols = pl.ds(pl.multiple_of((s * heads + h) * HD, HD), HD)
            pltpu.make_async_copy(sources[t].at[:, cols], mine, a_recv.at[h, t]).start()

    def whole_wait(ref, sem):
        pltpu.make_async_copy(ref, ref, sem).wait()

    def x_copy(h, t):
        return remote(
            kvb.at[t, h], kvx.at[t, h], x_send.at[h, t], x_recv.at[h, t], partner, s
        )

    def y_copy(h, t):
        return remote(
            kvx.at[t, h], kvy.at[t, h], y_send.at[h, t], y_recv.at[h, t], onward, s
        )

    def columns(place):
        return pl.ds(pl.multiple_of(place * HD, HD), HD)

    def g_copy(g, place, slot, recv, to):
        part = gat.at[g // 2, pl.ds(g % 2 * half, half), columns(place)]
        return remote(part, part, g_send.at[g, slot], recv, f, to)

    def own_copies(g):
        return [
            (z < chips - 1, g_copy(g, s, 0, g_recv.at[g, 0, 0], s + 2)),
            (z > 0, g_copy(g, s, 1, g_recv.at[g, 1, 0], s - 2)),
            (None, g_copy(g, s, 2, p_recv.at[g, z], mate)),
        ]

    def relay_copies(g, k):
        low, high = s - 2 * k, s + 2 * k
        base = 3 + 4 * (k - 1)
        copies = []
        if k < chips - 1:
            copies.append(((z >= k) & (z < chips - 1),
                           lambda: g_copy(g, low, base, g_recv.at[g, 0, k], s + 2)))
        copies.append((z >= k, lambda: g_copy(g, low, base + 1, p_recv.at[g, z - k], mate)))
        if k < chips - 1:
            copies.append(((z + k <= chips - 1) & (z > 0),
                           lambda: g_copy(g, high, base + 2, g_recv.at[g, 1, k], s - 2)))
        copies.append((z + k <= chips - 1,
                       lambda: g_copy(g, high, base + 3, p_recv.at[g, z + k], mate)))
        return copies

    def start_own(g):
        for cond, copy in own_copies(g):
            if cond is None:
                copy.start()
            else:
                pl.when(cond)(copy.start)

    def relay(g, k):
        @pl.when(z >= k)
        def _():
            g_copy(g, s - 2 * k, 0, g_recv.at[g, 0, k - 1], mate).wait_recv()

        @pl.when(z + k <= chips - 1)
        def _():
            g_copy(g, s + 2 * k, 0, g_recv.at[g, 1, k - 1], mate).wait_recv()

        for cond, make in relay_copies(g, k):
            @pl.when(cond)
            def _():
                make().start()

    near_pen = jnp.where(mask_ref[f, partner] == 1, 0.0, jnp.inf).astype(jnp.float32)
    far_pen = jnp.where(mask_ref[f, far] == 1, 0.0, jnp.inf).astype(jnp.float32)
    factor = math.log2(math.e) / math.sqrt(HD)
    q_tile = min(256, half)
    tiles = rows // q_tile

    def attend(h, first, last):
        def tile(i, carry):
            at = pl.ds(pl.multiple_of(i * q_tile, q_tile), q_tile)
            q = qb[h, at, :]
            places_kv = ((kvb, None), (kvx, near_pen), (kvy, far_pen))
            scores = []
            top = None
            for ref, pen in places_kv:
                sc = lax.dot_general(
                    q, ref[0, h], (((1,), (1,)), ((), ())),
                    preferred_element_type=jnp.float32,
                )
                scores.append(sc)
                best = jnp.max(sc, axis=1, keepdims=True)
                best = best if pen is None else best - pen
                top = best if top is None else jnp.maximum(top, best)
            total = None
            mixed = None
            for sc, (ref, pen) in zip(scores, places_kv):
                level = top if pen is None else top + pen
                e = jnp.exp2((sc - level) * factor)
                part = jnp.sum(e, axis=1, keepdims=True)
                prod = jnp.dot(
                    e.astype(jnp.bfloat16), ref[1, h], preferred_element_type=jnp.float32
                )
                total = part if total is None else total + part
                mixed = prod if mixed is None else mixed + prod
            gat[h, at, columns(s)] = (mixed / total).astype(jnp.bfloat16)
            return carry

        lax.fori_loop(first, last, tile, 0)

    p_tile = min(256, half)

    def project(c):
        g = c // 2
        for o in range(chips):
            g_copy(c, 2 * o + 1 - core, 0, p_recv.at[c, o], mate).wait_recv()
        if c % 2 == 0:
            whole_wait(wv.at[g], w_sem.at[g])

        def tile(i, carry):
            at = pl.ds(pl.multiple_of(c % 2 * half + i * p_tile, p_tile), p_tile)
            prod = jnp.dot(gat[g, at, :], wv[g], preferred_element_type=jnp.float32)
            if g > 0:
                prod = prod + acc[at, :]
            if g == heads - 1:
                out_ref[at, :] = prod.astype(out_ref.dtype)
            else:
                acc[at, :] = prod
            return carry

        lax.fori_loop(0, half // p_tile, tile, 0)

    chunks = 2 * heads
    events = sorted(
        ((c // 2 + k, c, k) for c in range(chunks) for k in range(1, chips))
    )
    done = [0]
    sent = set()
    ready = []

    def send_own(c):
        start_own(c)
        sent.add(c)

    def relay_upto(rank):
        while done[0] < len(events):
            key, c, k = events[done[0]]
            if key > rank or c not in sent:
                return
            relay(c, k)
            done[0] += 1
            if k == chips - 1:
                ready.append(c)

    for h in range(min(2, heads)):
        send_head(h)
    for h in range(heads):
        def load(i, carry):
            pltpu.make_async_copy(
                w_hbm.at[pl.ds(pl.multiple_of((i * heads + h) * HD, HD), HD), :],
                wv.at[h, pl.ds(pl.multiple_of(i * HD, HD), HD), :],
                w_sem.at[h],
            ).start()
            return carry

        lax.fori_loop(0, places, load, 0)

    for step in range(heads + 1):
        h = step - 1
        if step < heads:
            for t in range(2):
                whole_wait(kvb.at[t, step], a_recv.at[step, t])
                x_copy(step, t).start()
            if step + 2 < heads:
                send_head(step + 2)
        if h >= 0:
            whole_wait(qb.at[h], a_recv.at[h, 2])
            for t in range(2):
                y_copy(h, t).wait_recv()
            attend(h, 0, tiles // 2)
            send_own(2 * h)
        if step < heads:
            for t in range(2):
                x_copy(step, t).wait_recv()
                y_copy(step, t).start()
        if h >= heads - 2:
            relay_upto(1 if h == heads - 2 else 3)
        if h >= 0:
            attend(h, tiles // 2, tiles)
            send_own(2 * h + 1)
        if h == heads - 2:
            relay_upto(2)
    while done[0] < len(events):
        key = events[done[0]][0]
        if key == events[-1][0]:
            key, c, k = events[done[0]]
            relay(c, k)
            done[0] += 1
            ready.append(c)
        else:
            relay_upto(key)
        while ready:
            project(ready.pop(0))

    for h in range(heads):
        for t in range(3):
            part = landing(t, h).at[pl.ds(0, (places - 1) * tok), :]
            whole_wait(part, a_send.at[h, t])
        for t in range(2):
            x_copy(h, t).wait_send()
            y_copy(h, t).wait_send()
    for c in range(chunks):
        for cond, copy in own_copies(c):
            if cond is None:
                copy.wait_send()
            else:
                pl.when(cond)(copy.wait_send)
        for k in range(1, chips):
            for cond, make in relay_copies(c, k):
                @pl.when(cond)
                def _():
                    make().wait_send()


def solution(mesh):
    frames = mesh.shape["tm"]
    places = mesh.shape["space"]

    def body(queries, key_vectors, value_vectors, out_weight, frame_mask):
        tok, width = queries.shape
        heads = width // HD // places
        rows = tok * places
        chips = places // 2
        cols = out_weight.shape[1]
        bf16 = jnp.bfloat16
        anyspace = pl.BlockSpec(memory_space=pl.ANY)
        dma = pltpu.SemaphoreType.DMA
        return pl.pallas_call(
            functools.partial(kernel, frames, places, heads),
            out_shape=jax.ShapeDtypeStruct((rows, cols), bf16),
            in_specs=[anyspace] * 4 + [pl.BlockSpec(memory_space=pltpu.SMEM)],
            out_specs=pl.BlockSpec(memory_space=pltpu.VMEM),
            scratch_shapes=[
                pltpu.VMEM((heads, rows, HD), bf16),
                pltpu.VMEM((2, heads, rows, HD), bf16),
                pltpu.VMEM((2, heads, rows, HD), bf16),
                pltpu.VMEM((2, heads, rows, HD), bf16),
                pltpu.VMEM((heads, rows, places * HD), bf16),
                pltpu.VMEM((heads, places * HD, cols), bf16),
                pltpu.VMEM((rows, cols), jnp.float32),
                dma((heads, 3)), dma((heads, 3)),
                dma((heads, 2)), dma((heads, 2)),
                dma((heads, 2)), dma((heads, 2)),
                dma((2 * heads, 3 + 4 * (chips - 1))),
                dma((2 * heads, 2, chips - 1)),
                dma((2 * heads, chips)),
                dma((heads,)),
            ],
            compiler_params=pltpu.CompilerParams(
                collective_id=0, has_side_effects=True,
                vmem_limit_bytes=60 * 1024 * 1024,
            ),
        )(queries, key_vectors, value_vectors, out_weight, frame_mask)

    in_specs = (
        P(("tm", "space"), None),
        P(("tm", "space"), None),
        P(("tm", "space"), None),
        P(None, "space"),
        P(),
    )
    return jax.shard_map(
        body, mesh=mesh, in_specs=in_specs, out_specs=P("tm", "space"), check_vma=False
    )
```
